512 devices in a mesh: row: 32 (over x_lo, z), col: 16 (over x_hi, y, core).
Axes of the slice: x: 4 (x_hi: 2, x_lo: 2; x = x_hi * 2 + x_lo), y: 4, z: 16, core: 2. Of those that a mesh axis runs over, the one named last changes fastest.
Arguments:
- tokens: bfloat16 [256, 12288], P('row', 'col'), may hold values from -6 to 6
- past_tokens: bfloat16 [256, 12288], P('row', 'col'), may hold values from -6 to 6
- out_grad: bfloat16 [256, 12288], P('row', 'col'), may hold values from -3 to 3
- w_in: bfloat16 [12288, 24576], P('col', 'row'), may hold values from -0.0546875 to 0.0546875
- w_out: bfloat16 [24576, 12288], P('row', 'col'), may hold values from -0.0390625 to 0.0390625
Outputs:
- layer_out: bfloat16 [256, 12288], P('row', 'col')
- input_grad: bfloat16 [256, 12288], P('row', 'col')
- grad_w_in: bfloat16 [12288, 24576], P('col', 'row')
- grad_w_out: bfloat16 [24576, 12288], P('row', 'col')
The draws below stay inside these ranges and needn't reach their ends.
All inputs are finite; a program needn't handle non-finite values.
Results may differ from the reference program's by a relative error of at most 0.005.
Values may be sent and summed in bfloat16 or wider, within the bound.
A program may use at most 64 MiB of HBM per device.

```python
import jax
import jax.numpy as jnp

D = 12288
FF = 24576
TOKENS = 256


def steps_of(rng, extent, pieces, least, high):
    level, own = 1.0, jax.random.fold_in(rng, 6)
    for position, parts in pieces:
        draws = jnp.exp(jax.random.uniform(jax.random.fold_in(own, position), (parts,), jnp.float32, least / len(pieces), high / len(pieces)))
        level = level * jnp.repeat(draws, extent[position] // parts).reshape([-1 if axis == position else 1 for axis in range(len(extent))])
    return level


def centred(own_key, shape, spread, reach, shards=(), kind=jnp.bfloat16):
    result = jax.random.normal(own_key, shape, jnp.float32) * spread
    if len(shards) > 0:
        result = steps_of(own_key, shape, shards, -0.22, 0.18) * result
    return jnp.clip(result, min=-reach, max=reach).astype(kind)


def setup_inputs(seed: int = 0) -> dict:
    streams_of = jax.random.split(jax.random.key(seed), 6)
    tokens = centred(streams_of[0], (TOKENS, D), 1.0, 6.0, ((0, 32), (1, 16)))
    past_tokens = centred(streams_of[1], (TOKENS, D), 1.0, 6.0, ((0, 32), (1, 16)))
    out_grad = centred(streams_of[2], (TOKENS, D), 0.5, 3.0, ((0, 32), (1, 16)))
    w_in = centred(streams_of[3], (D, FF), D ** -0.5, 0.0546875, ((0, 16), (1, 32)))
    w_out = centred(streams_of[4], (FF, D), FF ** -0.5, 0.0390625, ((0, 32), (1, 16)))
    return {"tokens": tokens, "past_tokens": past_tokens, "out_grad": out_grad, "w_in": w_in, "w_out": w_out}


def gelu_parts(pre):
    cdf = 0.5 * (1.0 + jax.scipy.special.erf(pre * 0.7071067811865476))
    slope = cdf + pre * jnp.exp(-0.5 * pre * pre) * 0.3989422804014327
    return pre * cdf, slope


def reference(tokens, past_tokens, out_grad, w_in, w_out):
    pre = jnp.dot(tokens, w_in, preferred_element_type=jnp.float32)
    hidden = gelu_parts(pre)[0].astype(jnp.bfloat16)
    layer_out = jnp.dot(hidden, w_out, preferred_element_type=jnp.float32).astype(jnp.bfloat16)
    past_pre = jnp.dot(past_tokens, w_in, preferred_element_type=jnp.float32)
    past_act, slope = gelu_parts(past_pre)
    past_hidden = past_act.astype(jnp.bfloat16)
    back = jnp.dot(out_grad, w_out.T, preferred_element_type=jnp.float32)
    hidden_grad = (back * slope).astype(jnp.bfloat16)
    grad_w_out = jnp.dot(past_hidden.T, out_grad, preferred_element_type=jnp.float32).astype(jnp.bfloat16)
    grad_w_in = jnp.dot(past_tokens.T, hidden_grad, preferred_element_type=jnp.float32).astype(jnp.bfloat16)
    input_grad = jnp.dot(hidden_grad, w_in.T, preferred_element_type=jnp.float32).astype(jnp.bfloat16)
    return layer_out, input_grad, grad_w_in, grad_w_out
```

```python
import functools

import jax
import jax.numpy as jnp
from jax import lax
from jax.experimental import pallas as pl
from jax.experimental.pallas import tpu as pltpu
from jax.sharding import PartitionSpec as P

MESH = pl.DeviceIdType.MESH
F32, BF16 = jnp.float32, jnp.bfloat16
NZ = 16


def gelu_parts(pre):
    cdf = 0.5 * (1.0 + lax.erf(pre * 0.7071067811865476))
    slope = cdf + pre * jnp.exp(-0.5 * pre * pre) * 0.3989422804014327
    return (pre * cdf, slope)


LANES = ((0, 0), (1, 0), (2, 0), (2, 1))
FAR = (0, 1, 0, 1)


def kernel(
    past_ref, grad_ref, tok_ref, win_hbm, wout_hbm,
    lay_ref, ing_ref, pall_ref, gall_ref, aall_ref, hall_ref,
    T, win, wout, Pf, Pb, Dr, S8, Cs, Cr, H,
    Rf, Xb, Xr, Sf, Sb, R1, Uf, Ub, R2,
    wsem, azs, azr, axs, axr, lsem,
    dss, drs, css, crs, hss, hrs, hds, hdr,
    xss, xrs, s1s, s1r, s2s, s2r,
):
    r, q = lax.axis_index("row"), lax.axis_index("col")
    xl, z = r // NZ, r % NZ
    ch, c = q // 2, q % 2
    xh, y = ch // 4, ch % 4
    xp = (1 - xl) * NZ + z
    qp = ch * 2 + (1 - c)

    def zrow(d):
        return xl * NZ + (z + d + NZ) % NZ

    def chip(k, sign=1):
        return ((xh + sign * (k // 4) + 2) % 2) * 4 + (y + sign * (k % 4) + 4) % 4

    def rcopy(src, dst, ss, rs, rr, qq):
        return pltpu.make_async_remote_copy(
            src_ref=src, dst_ref=dst, send_sem=ss, recv_sem=rs, device_id=(rr, qq), device_id_type=MESH
        )

    cw1 = pltpu.make_async_copy(win_hbm, win, wsem.at[0])
    cw2 = pltpu.make_async_copy(wout_hbm, wout, wsem.at[1])
    cw1.start()
    cw2.start()
    own = (past_ref, grad_ref, tok_ref)
    locs = [pltpu.make_async_copy(own[a], T.at[a, r], lsem.at[a]) for a in range(3)]
    for cp in locs:
        cp.start()

    barrier = pltpu.get_barrier_semaphore()
    rows = [zrow(d) for d in (1, -1, 2, -2, 4, -4, 8)] + [xp]
    for rr in rows:
        pl.semaphore_signal(barrier, inc=1, device_id=(rr, q), device_id_type=MESH)
    for qq in [chip(k) * 2 + c for k in range(1, 8)] + [qp]:
        pl.semaphore_signal(barrier, inc=1, device_id=(r, qq), device_id_type=MESH)
    pl.semaphore_wait(barrier, 16)

    def xcopy(src, a, slot_z, slot):
        return rcopy(src, T.at[a, slot], axs.at[a, slot_z], axr.at[a, slot_z], xp, q)

    def zcopy(src, a, slot, di, s, ln):
        return rcopy(src, T.at[a, slot], azs.at[di, s, ln], azr.at[di, s + 1, ln], zrow(1 - 2 * di), q)

    for a in (2, 0, 1):
        xcopy(own[a], a, z, r).start()
    for ln, (a, h) in enumerate(LANES):
        if h == 0:
            for di in range(2):
                zcopy(own[a], a, r, di, 0, ln).start()
    for ln, (a, h) in enumerate(LANES):
        if h == 1:
            xcopy(T.at[a, xp], a, z, xp).wait_recv()
            for di in range(2):
                zcopy(T.at[a, xp], a, xp, di, 0, ln).start()

    def arrive(s, far):
        for di in range(2):
            zz = (z - (1 - 2 * di) * s + 2 * NZ) % NZ
            for ln, (a, h) in enumerate(LANES):
                if far == 2 and FAR[ln] != di:
                    continue
                slot = (xl if h == 0 else 1 - xl) * NZ + zz
                zcopy(T.at[a, slot], a, slot, di, s - 1, ln).wait_recv()
                if far == 0 or (far == 1 and FAR[ln] == di):
                    zcopy(T.at[a, slot], a, slot, di, s, ln).start()
                if h == 0 and a != 2:
                    xcopy(T.at[a, slot], a, zz, slot).start()

    @pl.loop(1, 7)
    def _(s):
        arrive(s, 0)

    arrive(7, 1)
    arrive(8, 2)

    cw1.wait()
    cw2.wait()
    for cp in locs:
        cp.wait()

    def wait_x(a):
        @pl.loop(0, NZ)
        def _(zz):
            slot = (1 - xl) * NZ + zz
            xcopy(T.at[a, slot], a, zz, slot).wait_recv()

    def gathered(a):
        return T[a].astype(F32).reshape(256, 768).astype(BF16)

    def d2d(k):
        return rcopy(Pb.at[k, :, 1 - c], Dr.at[k], dss.at[k], drs.at[k], r, qp)

    def partial(k, part):
        part = part.reshape(8, 2, 16, 768)
        Pf[k] = part
        Pb[k] = part.astype(BF16)
        d2d(k).start()

    wait_x(0)
    x = gathered(0)
    pall_ref[...] = x
    partial(0, jnp.dot(x, win[...], preferred_element_type=F32))
    wait_x(1)
    x = gathered(1)
    gall_ref[...] = x
    partial(1, lax.dot_general(x, wout[...], (((1,), (1,)), ((), ())), preferred_element_type=F32))
    partial(2, jnp.dot(gathered(2), win[...], preferred_element_type=F32))

    def csend(k, j):
        return rcopy(Cs.at[k, chip(j)], Cr.at[k, j], css.at[k, j], crs.at[k, j], r, chip(j) * 2 + c)

    for k in range(3):
        d2d(k).wait_recv()
        sums = Pf[k, :, c] + Dr[k].astype(F32)
        S8[k] = sums
        Cs[k] = sums.astype(BF16)
        for j in range(1, 8):
            csend(k, j).start()

    def summed(k):
        total = S8[k, ch]
        for j in range(1, 8):
            csend(k, j).wait_recv()
        for j in range(1, 8):
            total = total + Cr[k, j].astype(F32)
        return total

    def hsend(k, j):
        return rcopy(H.at[k, ch, c], H.at[k, ch, c], hss.at[k, j], hrs.at[k, j], r, chip(j) * 2 + c)

    def hpass(k, j):
        src = H.at[k, chip(j, -1), c]
        return rcopy(src, src, hds.at[k, j], hdr.at[k, j], r, qp)

    def hpassed(k, j):
        src = H.at[k, chip(j, -1), 1 - c]
        return rcopy(src, src, hds.at[k, j], hdr.at[k, j], r, qp)

    def hrecv(k, j):
        src = H.at[k, chip(j, -1), c]
        return rcopy(src, src, hss.at[k, j], hrs.at[k, j], r, qp)

    def spread(k, value):
        H[k, ch, c] = value
        for j in range(1, 8):
            hsend(k, j).start()
        hpass(k, 0).start()

    act, slope = gelu_parts(summed(0))
    spread(0, act.astype(BF16))
    spread(1, (summed(1) * slope).astype(BF16))
    spread(2, gelu_parts(summed(2))[0].astype(BF16))
    for k in range(3):
        for j in (1, 3, 4, 2, 5, 7, 6):
            hrecv(k, j).wait_recv()
            hpass(k, j).start()

    def whole(k):
        for j in range(8):
            hpassed(k, j).wait_recv()
        return H[k].reshape(256, 768)

    def xsend(k):
        return rcopy(Xb.at[k, 1 - xl], Xr.at[k], xss.at[k], xrs.at[k], xp, q)

    def rpartial(k, part):
        part = part.reshape(2, NZ, 8, 768)
        Rf[k] = part
        Xb[k] = part.astype(BF16)
        xsend(k).start()

    aall_ref[...] = whole(0)
    x = whole(1)
    hall_ref[...] = x
    rpartial(0, lax.dot_general(x, win[...], (((1,), (1,)), ((), ())), preferred_element_type=F32))
    rpartial(1, jnp.dot(whole(2), wout[...], preferred_element_type=F32))

    STEP1 = ((1, -1, 2), (1, -1, -2))

    def send1(k, i):
        d = STEP1[k][i]
        return rcopy(Sb.at[k, :, (z + d + NZ) % 4], R1.at[k, i], s1s.at[k, i], s1r.at[k, i], zrow(d), q)

    for k in range(2):
        xsend(k).wait_recv()
        s = Rf[k, xl] + Xr[k].astype(F32)
        s = s.reshape(4, 4, 8, 768)
        Sf[k] = s
        Sb[k] = s.astype(BF16)
        for i in range(3):
            send1(k, i).start()

    def send2(k, i):
        d = 4 * i
        return rcopy(Ub.at[k, ((z + d) % NZ) // 4], R2.at[k, i], s2s.at[k, i], s2r.at[k, i], zrow(d), q)

    for k in range(2):
        u = Sf[k, :, z % 4]
        for i in range(3):
            send1(k, i).wait_recv()
        for i in range(3):
            u = u + R1[k, i].astype(F32)
        Uf[k] = u
        Ub[k] = u.astype(BF16)
        for i in range(1, 4):
            send2(k, i).start()

    outs = (ing_ref, lay_ref)
    for k in range(2):
        v = Uf[k, z // 4]
        for i in range(1, 4):
            send2(k, i).wait_recv()
        for i in range(1, 4):
            v = v + R2[k, i].astype(F32)
        outs[k][...] = v.astype(BF16)

    for k in range(2):
        xsend(k).wait_send()
        for i in range(3):
            send1(k, i).wait_send()
            send2(k, i + 1).wait_send()
    for k in range(3):
        d2d(k).wait_send()
        for j in range(1, 8):
            csend(k, j).wait_send()
            hsend(k, j).wait_send()
        for j in range(8):
            hpass(k, j).wait_send()
    for a in range(2):
        @pl.loop(0, NZ)
        def _(zz):
            slot = xl * NZ + zz
            xcopy(T.at[a, slot], a, zz, slot).wait_send()
    xcopy(T.at[2, r], 2, z, r).wait_send()

    for ln, (a, h) in enumerate(LANES):
        for di in range(2):
            n = 8 if FAR[ln] == di else 7

            @pl.loop(0, n)
            def _(s):
                zcopy(T.at[a, r], a, r, di, s, ln).wait_send()


def call(past, grad, tok, win, wout):
    vm = pl.BlockSpec(memory_space=pltpu.VMEM)
    hbm = pl.BlockSpec(memory_space=pl.ANY)
    V = pltpu.VMEM
    D = lambda *s: pltpu.SemaphoreType.DMA(s)
    blk = jax.ShapeDtypeStruct((8, 768), BF16)
    full = jax.ShapeDtypeStruct((256, 768), BF16)
    return pl.pallas_call(
        kernel,
        out_shape=(blk, blk, full, full, full, full),
        in_specs=[vm, vm, vm, hbm, hbm],
        out_specs=(vm,) * 6,
        scratch_shapes=[
            V((3, 32, 8, 768), BF16), V((768, 768), BF16), V((768, 768), BF16),
            V((3, 8, 2, 16, 768), F32), V((3, 8, 2, 16, 768), BF16), V((3, 8, 16, 768), BF16),
            V((3, 8, 16, 768), F32), V((3, 8, 16, 768), BF16), V((3, 8, 16, 768), BF16),
            V((3, 8, 2, 16, 768), BF16),
            V((2, 2, 16, 8, 768), F32), V((2, 2, 16, 8, 768), BF16), V((2, 16, 8, 768), BF16),
            V((2, 4, 4, 8, 768), F32), V((2, 4, 4, 8, 768), BF16), V((2, 3, 4, 8, 768), BF16),
            V((2, 4, 8, 768), F32), V((2, 4, 8, 768), BF16), V((2, 4, 8, 768), BF16),
            D(2), D(2, 9, 4), D(2, 9, 4), D(3, 16), D(3, 16), D(3),
            D(3), D(3), D(3, 8), D(3, 8), D(3, 8), D(3, 8), D(3, 8), D(3, 8),
            D(2), D(2), D(2, 3), D(2, 3), D(2, 4), D(2, 4),
        ],
        compiler_params=pltpu.CompilerParams(
            collective_id=0, has_side_effects=True, vmem_limit_bytes=56 * 1024 * 1024
        ),
        name="ffn",
    )(past, grad, tok, win, wout)


def local(tokens, past_tokens, out_grad, w_in, w_out):
    lay, ing, past_all, grad_all, act_all, hid_all = call(past_tokens, out_grad, tokens, w_in, w_out)
    tn = (((0,), (0,)), ((), ()))
    grad_w_out = lax.dot_general(act_all, grad_all, tn, preferred_element_type=F32).astype(BF16)
    grad_w_in = lax.dot_general(past_all, hid_all, tn, preferred_element_type=F32).astype(BF16)
    return (lay, ing, grad_w_in, grad_w_out)


def solution(mesh):
    return jax.shard_map(
        local,
        mesh=mesh,
        in_specs=(P("row", "col"), P("row", "col"), P("row", "col"), P("col", "row"), P("row", "col")),
        out_specs=(P("row", "col"), P("row", "col"), P("col", "row"), P("row", "col")),
        check_vma=False,
    )
```

```python
import functools

import jax
import jax.numpy as jnp
from jax import lax
from jax.experimental import pallas as pl
from jax.experimental.pallas import tpu as pltpu
from jax.sharding import PartitionSpec as P

MESH = pl.DeviceIdType.MESH
F32, BF16 = jnp.float32, jnp.bfloat16
NZ = 16


def gelu_parts(pre):
    cdf = 0.5 * (1.0 + lax.erf(pre * 0.7071067811865476))
    slope = cdf + pre * jnp.exp(-0.5 * pre * pre) * 0.3989422804014327
    return (pre * cdf, slope)


SEED = (0, 4, -4, 8)
SPREAD = ((1, 0), (-1, 0), (2, 0), (-2, 0), (1, 1), (-1, 1), (2, 1), (1, 2), (-1, 2), (-2, 2), (1, 3), (-1, 3))


def kernel(
    past_hbm, grad_hbm, tok_hbm, win_hbm, wout_hbm,
    lay_ref, ing_ref, gwi, gwo,
    T, win, wout, Pf, Dr, S8, Cs, Cr, H,
    Rf, Xb, Xr, Sf, Sb, R1, Uf, Ub, R2,
    wsem, ass, asr, bss, bsr, axs, axr, lsem,
    dss, drs, css, crs, hss, hrs, hds, hdr,
    xss, xrs, s1s, s1r, s2s, s2r,
):
    r, q = lax.axis_index("row"), lax.axis_index("col")
    xl, z = r // NZ, r % NZ
    ch, c = q // 2, q % 2
    xh, y = ch // 4, ch % 4
    xp = (1 - xl) * NZ + z
    qp = ch * 2 + (1 - c)
    last = []

    def zrow(d, x=xl):
        return x * NZ + (z + d + 2 * NZ) % NZ

    def chip(k, sign=1):
        return ((xh + sign * (k // 4) + 2) % 2) * 4 + (y + sign * (k % 4) + 4) % 4

    def rcopy(src, dst, ss, rs, rr, qq):
        return pltpu.make_async_remote_copy(
            src_ref=src, dst_ref=dst, send_sem=ss, recv_sem=rs, device_id=(rr, qq), device_id_type=MESH
        )

    def go(cp):
        cp.start()
        last.append(cp.wait_send)

    own = (past_hbm, grad_hbm, tok_hbm)
    locs = [pltpu.make_async_copy(own[a], T.at[a, r], lsem.at[a]) for a in range(3)]
    for cp in locs:
        cp.start()
    cw1 = pltpu.make_async_copy(win_hbm, win, wsem.at[0])
    cw2 = pltpu.make_async_copy(wout_hbm, wout, wsem.at[1])
    cw1.start()
    cw2.start()

    barrier = pltpu.get_barrier_semaphore()
    rows = [zrow(d) for d in (1, -1, 2, -2, 4, -4)] + [xp]
    for rr in rows:
        pl.semaphore_signal(barrier, inc=1, device_id=(rr, q), device_id_type=MESH)
    for qq in [chip(k) * 2 + c for k in range(1, 8)] + [qp]:
        pl.semaphore_signal(barrier, inc=1, device_id=(r, qq), device_id_type=MESH)
    pl.semaphore_wait(barrier, 15)

    def xcopy(src, a, d):
        zz = (z + d + 2 * NZ) % NZ
        slot = xl * NZ + zz
        return rcopy(src, T.at[a, slot], axs.at[a, zz], axr.at[a, zz], xp, q)

    def acopy(src, a, e, e2, d):
        slot = zrow(SEED[e])
        return rcopy(src, T.at[a, slot], ass.at[a, e2], asr.at[a, e2], zrow(d), q)

    def arecv(a, e2):
        slot = zrow(SEED[e2])
        acopy(T.at[a, slot], a, e2, e2, 4).wait_recv()

    def bcopy(src, a, i):
        d, e = SPREAD[i]
        slot = zrow(SEED[e])
        return rcopy(src, T.at[a, slot], bss.at[a, i], bsr.at[a, i], zrow(-d), q)

    def brecv(a, i):
        d, e = SPREAD[i]
        slot = zrow(d + SEED[e])
        rcopy(T.at[a, slot], T.at[a, slot], bss.at[a, i], bsr.at[a, i], zrow(-d), q).wait_recv()
        go(xcopy(T.at[a, slot], a, d + SEED[e]))

    def seeded(a, e):
        src = T.at[a, zrow(SEED[e])]
        if e == 0:
            go(acopy(src, a, 0, 1, -4))
            go(acopy(src, a, 0, 2, 4))
        far = 1 + a % 2
        if e == far:
            go(acopy(src, a, e, 3, -SEED[e]))
        for i, (d, e2) in enumerate(SPREAD):
            if e2 == e:
                go(bcopy(src, a, i))
        go(xcopy(src, a, SEED[e]))

    def spread_of(a, es):
        for i, (d, e) in enumerate(SPREAD):
            if e in es:
                brecv(a, i)

    for a in range(3):
        locs[a].wait()
        seeded(a, 0)
    for a in range(3):
        spread_of(a, (0,))
    for a in range(3):
        for e in (1, 2):
            arecv(a, e)
            seeded(a, e)
    for a in range(3):
        arecv(a, 3)
        seeded(a, 3)
    for a in range(2):
        spread_of(a, (1, 2))
    for a in range(2):
        spread_of(a, (3,))

    cw1.wait()
    cw2.wait()

    def gathered(a):
        @pl.loop(0, NZ)
        def _(zz):
            slot = (1 - xl) * NZ + zz
            rcopy(T.at[a, slot], T.at[a, slot], axs.at[a, zz], axr.at[a, zz], xp, q).wait_recv()

        return T[a].astype(F32).reshape(256, 768).astype(BF16)

    def d2d(k):
        return rcopy(Pf.at[k, :, 1 - c], Dr.at[k], dss.at[k], drs.at[k], r, qp)

    def partial(k, part):
        Pf[k] = part.reshape(8, 2, 16, 768)
        go(d2d(k))

    def csend(k, j):
        return rcopy(Cs.at[k, chip(j)], Cr.at[k, j], css.at[k, j], crs.at[k, j], r, chip(j) * 2 + c)

    def scatter(k):
        d2d(k).wait_recv()
        sums = Pf[k, :, c] + Dr[k]
        S8[k] = sums
        Cs[k] = sums.astype(BF16)
        for j in (6, 2, 4, 5, 7, 1, 3):
            go(csend(k, j))

    def summed(k):
        total = S8[k, ch]
        for j in range(1, 8):
            csend(k, j).wait_recv()
        for j in range(1, 8):
            total = total + Cr[k, j].astype(F32)
        return total

    def hcopy(k, owner, j, ss, rs, core, qq):
        ref = H.at[k, owner, core]
        return rcopy(ref, ref, ss.at[k, j], rs.at[k, j], r, qq)

    def spread(k, value):
        H[k, ch, c] = value
        for j in (6, 2, 4, 5, 7, 1, 3):
            go(hcopy(k, ch, j, hss, hrs, c, chip(j) * 2 + c))
        go(hcopy(k, ch, 0, hds, hdr, c, qp))

    def pass_on(k):
        for j in (1, 3, 4, 2, 5, 7, 6):
            hcopy(k, chip(j, -1), j, hss, hrs, c, qp).wait_recv()
            go(hcopy(k, chip(j, -1), j, hds, hdr, c, qp))

    def whole(k):
        for j in range(8):
            hcopy(k, chip(j, -1), j, hds, hdr, 1 - c, qp).wait_recv()
        return H[k].reshape(256, 768)

    def xsend(k):
        return rcopy(Xb.at[k, 1 - xl], Xr.at[k], xss.at[k], xrs.at[k], xp, q)

    def rpartial(k, part):
        part = part.reshape(2, NZ, 8, 768)
        Rf[k] = part
        Xb[k] = part.astype(BF16)
        go(xsend(k))

    STEP1 = ((2, 1, -1), (-2, 1, -1))

    def send1(k, i):
        d = STEP1[k][i]
        return rcopy(Sb.at[k, :, (z + d + NZ) % 4], R1.at[k, i], s1s.at[k, i], s1r.at[k, i], zrow(d), q)

    def row1(k):
        xsend(k).wait_recv()
        s = Rf[k, xl] + Xr[k].astype(F32)
        s = s.reshape(4, 4, 8, 768)
        Sf[k] = s
        Sb[k] = s.astype(BF16)
        for i in range(3):
            go(send1(k, i))

    def send2(k, i):
        d = 4 * i
        return rcopy(Ub.at[k, ((z + d) % NZ) // 4], R2.at[k, i], s2s.at[k, i], s2r.at[k, i], zrow(d), q)

    def row2(k):
        u = Sf[k, :, z % 4]
        for i in range(3):
            send1(k, i).wait_recv()
        for i in range(3):
            u = u + R1[k, i].astype(F32)
        Uf[k] = u
        Ub[k] = u.astype(BF16)
        for i in (2, 1, 3):
            go(send2(k, i))

    def row3(k, out_ref):
        v = Uf[k, z // 4]
        for i in range(1, 4):
            send2(k, i).wait_recv()
        for i in range(1, 4):
            v = v + R2[k, i].astype(F32)
        out_ref[...] = v.astype(BF16)

    tn = (((0,), (0,)), ((), ()))
    nt = (((1,), (1,)), ((), ()))
    x = gathered(0)
    partial(0, jnp.dot(x, win[...], preferred_element_type=F32))
    g = gathered(1)
    partial(1, lax.dot_general(g, wout[...], nt, preferred_element_type=F32))
    spread_of(2, (1, 2))
    scatter(0)
    scatter(1)
    spread_of(2, (3,))
    partial(2, jnp.dot(gathered(2), win[...], preferred_element_type=F32))
    act, slope = gelu_parts(summed(0))
    spread(0, act.astype(BF16))
    spread(1, (summed(1) * slope).astype(BF16))
    scatter(2)
    pass_on(0)
    pass_on(1)
    spread(2, gelu_parts(summed(2))[0].astype(BF16))
    h = whole(1)
    rpartial(0, lax.dot_general(h, win[...], nt, preferred_element_type=F32))
    pass_on(2)
    rpartial(1, jnp.dot(whole(2), wout[...], preferred_element_type=F32))
    gwi[...] = lax.dot_general(
        T[0].astype(F32).reshape(256, 768).astype(BF16), h, tn, preferred_element_type=F32
    ).astype(BF16)
    row1(0)
    gwo[...] = lax.dot_general(
        whole(0), T[1].astype(F32).reshape(256, 768).astype(BF16), tn, preferred_element_type=F32
    ).astype(BF16)
    row1(1)
    row2(0)
    row2(1)
    row3(0, ing_ref)
    row3(1, lay_ref)

    for wait in last:
        wait()


def call(past, grad, tok, win, wout):
    vm = pl.BlockSpec(memory_space=pltpu.VMEM)
    hbm = pl.BlockSpec(memory_space=pltpu.HBM)
    V = pltpu.VMEM
    D = lambda *s: pltpu.SemaphoreType.DMA(s)
    blk = jax.ShapeDtypeStruct((8, 768), BF16)
    wt = jax.ShapeDtypeStruct((768, 768), BF16)
    return pl.pallas_call(
        kernel,
        out_shape=(blk, blk, wt, wt),
        in_specs=[hbm] * 5,
        out_specs=(vm,) * 4,
        scratch_shapes=[
            V((3, 32, 8, 768), BF16), V((768, 768), BF16), V((768, 768), BF16),
            V((3, 8, 2, 16, 768), F32), V((3, 8, 16, 768), F32),
            V((3, 8, 16, 768), F32), V((3, 8, 16, 768), BF16), V((3, 8, 16, 768), BF16),
            V((3, 8, 2, 16, 768), BF16),
            V((2, 2, 16, 8, 768), F32), V((2, 2, 16, 8, 768), BF16), V((2, 16, 8, 768), BF16),
            V((2, 4, 4, 8, 768), F32), V((2, 4, 4, 8, 768), BF16), V((2, 3, 4, 8, 768), BF16),
            V((2, 4, 8, 768), F32), V((2, 4, 8, 768), BF16), V((2, 4, 8, 768), BF16),
            D(2), D(3, 4), D(3, 4), D(3, 12), D(3, 12), D(3, 16), D(3, 16), D(3),
            D(3), D(3), D(3, 8), D(3, 8), D(3, 8), D(3, 8), D(3, 8), D(3, 8),
            D(2), D(2), D(2, 3), D(2, 3), D(2, 4), D(2, 4),
        ],
        compiler_params=pltpu.CompilerParams(
            collective_id=0, has_side_effects=True, vmem_limit_bytes=36 * 1024 * 1024
        ),
        name="ffn",
    )(past, grad, tok, win, wout)


def local(tokens, past_tokens, out_grad, w_in, w_out):
    return call(past_tokens, out_grad, tokens, w_in, w_out)


def solution(mesh):
    return jax.shard_map(
        local,
        mesh=mesh,
        in_specs=(P("row", "col"), P("row", "col"), P("row", "col"), P("col", "row"), P("row", "col")),
        out_specs=(P("row", "col"), P("row", "col"), P("col", "row"), P("row", "col")),
        check_vma=False,
    )
```

```python
import functools

import jax
import jax.numpy as jnp
from jax import lax
from jax.experimental import pallas as pl
from jax.experimental.pallas import tpu as pltpu
from jax.sharding import PartitionSpec as P

MESH = pl.DeviceIdType.MESH
F32, BF16 = jnp.float32, jnp.bfloat16
NZ = 16


def gelu_parts(pre):
    cdf = 0.5 * (1.0 + lax.erf(pre * 0.7071067811865476))
    slope = cdf + pre * jnp.exp(-0.5 * pre * pre) * 0.3989422804014327
    return (pre * cdf, slope)


SEED = (0, 5, -5)
NEAR = tuple((d, e) for e in range(3) for d in (2, -2, 1, -1))
SPREAD = (NEAR + ((3, 1),), NEAR + ((-3, 2),), NEAR + ((3, 1),))
BOTH = (12,)
FOLD = tuple((d, m) for m in (5, -5, 0) for d in (2, -2, 1, -1))
FOLDS = (((-3, -5),) + FOLD, ((3, 5),) + FOLD)


def kernel(
    acts_ref, win_hbm, wout_hbm,
    lay_ref, ing_ref, gwi, gwo,
    T, win, wout, Pf, Dr, S8, Cs, Cr, H,
    Rf, Xb, Xr, Sf, Sb, R1, Ub, R2,
    wsem, ass, asr, bss, bsr, bds, axs, axr, lsem,
    dss, drs, css, crs, hss, hrs, hds, hdr,
    xss, xrs, s1s, s1r, s2s, s2r,
):
    r, q = lax.axis_index("row"), lax.axis_index("col")
    xl, z = r // NZ, r % NZ
    ch, c = q // 2, q % 2
    xh, y = ch // 4, ch % 4
    xp = (1 - xl) * NZ + z
    qp = ch * 2 + (1 - c)
    last = []

    def zrow(d, x=xl):
        return x * NZ + (z + d + 2 * NZ) % NZ

    def chip(k, sign=1):
        return ((xh + sign * (k // 4) + 2) % 2) * 4 + (y + sign * (k % 4) + 4) % 4

    def rcopy(src, dst, ss, rs, rr, qq):
        return pltpu.make_async_remote_copy(
            src_ref=src, dst_ref=dst, send_sem=ss, recv_sem=rs, device_id=(rr, qq), device_id_type=MESH
        )

    def go(cp):
        cp.start()
        last.append(cp.wait_send)

    loc = pltpu.make_async_copy(acts_ref, T.at[:, r], lsem.at[0])
    loc.start()
    cw1 = pltpu.make_async_copy(win_hbm, win, wsem.at[0])
    cw2 = pltpu.make_async_copy(wout_hbm, wout, wsem.at[1])
    cw1.start()
    cw2.start()

    barrier = pltpu.get_barrier_semaphore()
    rows = [zrow(d) for d in (1, -1, 2, -2, 3, -3, 5, -5)] + [zrow(d, 1 - xl) for d in (0, 2, -2, 3, -3)]
    for rr in rows:
        pl.semaphore_signal(barrier, inc=1, device_id=(rr, q), device_id_type=MESH)
    for qq in [chip(k) * 2 + c for k in range(1, 8)] + [qp]:
        pl.semaphore_signal(barrier, inc=1, device_id=(r, qq), device_id_type=MESH)
    pl.semaphore_wait(barrier, 21)

    def xcopy(src, a, d):
        zz = (z + d + 2 * NZ) % NZ
        slot = xl * NZ + zz
        return rcopy(src, T.at[a, slot], axs.at[a, zz], axr.at[a, zz], xp, q)

    def acopy(src, a, e, e2, d):
        slot = zrow(SEED[e])
        return rcopy(src, T.at[a, slot], ass.at[a, e2], asr.at[a, e2], zrow(d), q)

    def arecv(a, e2):
        slot = zrow(SEED[e2])
        acopy(T.at[a, slot], a, e2, e2, 5).wait_recv()

    def bcopy(src, a, i):
        d, e = SPREAD[a][i]
        slot = zrow(SEED[e])
        return rcopy(src, T.at[a, slot], bss.at[a, i], bsr.at[a, i], zrow(-d), q)

    def bcross(src, a, i):
        d, e = SPREAD[a][i]
        zz = (z + SEED[e] + 2 * NZ) % NZ
        slot = zrow(SEED[e])
        return rcopy(src, T.at[a, slot], bds.at[a, i], axr.at[a, zz], zrow(-d, 1 - xl), q)

    def brecv(a, i):
        d, e = SPREAD[a][i]
        slot = zrow(d + SEED[e])
        rcopy(T.at[a, slot], T.at[a, slot], bss.at[a, i], bsr.at[a, i], zrow(-d), q).wait_recv()
        if i not in BOTH:
            go(xcopy(T.at[a, slot], a, d + SEED[e]))

    def seeded(a, e):
        src = acts_ref.at[a] if e == 0 else T.at[a, zrow(SEED[e])]
        if e == 0:
            go(acopy(src, a, 0, 1, -5))
            go(acopy(src, a, 0, 2, 5))
        for i in sorted(range(13), key=lambda i: -abs(SPREAD[a][i][0])):
            if SPREAD[a][i][1] == e:
                go(bcopy(src, a, i))
                if i in BOTH:
                    go(bcross(src, a, i))
        go(xcopy(src, a, SEED[e]))

    def spread_of(a, es):
        for i, (d, e) in enumerate(SPREAD[a]):
            if e in es:
                brecv(a, i)

    for a in range(2):
        seeded(a, 0)
    for a in range(2):
        spread_of(a, (0,))
    for a in range(2):
        for e in (1, 2):
            arecv(a, e)
            seeded(a, e)
    seeded(2, 0)
    for a in range(2):
        spread_of(a, (1, 2))
    spread_of(2, (0,))
    for e in (1, 2):
        arecv(2, e)
        seeded(2, e)

    cw1.wait()
    cw2.wait()
    loc.wait()

    def gathered(a):
        @pl.loop(0, NZ)
        def _(zz):
            slot = (1 - xl) * NZ + zz
            rcopy(T.at[a, slot], T.at[a, slot], axs.at[a, zz], axr.at[a, zz], xp, q).wait_recv()

        return T[a].astype(F32).reshape(256, 768).astype(BF16)

    def d2d(k):
        return rcopy(Pf.at[k, :, 1 - c], Dr.at[k], dss.at[k], drs.at[k], r, qp)

    def partial(k, part):
        Pf[k] = part.reshape(8, 2, 16, 768)
        go(d2d(k))

    def csend(k, j):
        return rcopy(Cs.at[k, chip(j)], Cr.at[k, j], css.at[k, j], crs.at[k, j], r, chip(j) * 2 + c)

    def scatter(k):
        d2d(k).wait_recv()
        sums = Pf[k, :, c] + Dr[k]
        S8[k] = sums
        Cs[k] = sums.astype(BF16)
        for j in (6, 2, 4, 5, 7, 1, 3):
            go(csend(k, j))

    def summed(k):
        total = S8[k, ch]
        for j in range(1, 8):
            csend(k, j).wait_recv()
        for j in range(1, 8):
            total = total + Cr[k, j].astype(F32)
        return total

    def hcopy(k, owner, j, ss, rs, core, qq):
        ref = H.at[k, owner, core]
        return rcopy(ref, ref, ss.at[k, j], rs.at[k, j], r, qq)

    def spread(k, value):
        H[k, ch, c] = value
        for j in (6, 2, 4, 5, 7, 1, 3):
            go(hcopy(k, ch, j, hss, hrs, c, chip(j) * 2 + c))
        go(hcopy(k, ch, 0, hds, hdr, c, qp))

    def pass_on(k):
        for j in (1, 3, 4, 2, 5, 7, 6):
            hcopy(k, chip(j, -1), j, hss, hrs, c, qp).wait_recv()
            go(hcopy(k, chip(j, -1), j, hds, hdr, c, qp))

    def whole(k):
        for j in range(8):
            hcopy(k, chip(j, -1), j, hds, hdr, 1 - c, qp).wait_recv()
        return H[k].reshape(256, 768)

    def xsend(k):
        return rcopy(Xb.at[k, 1 - xl], Xr.at[k], xss.at[k], xrs.at[k], xp, q)

    def rpartial(k, part):
        part = part.reshape(2, NZ, 8, 768)
        Rf[k] = part
        Xb[k] = part.astype(BF16)
        go(xsend(k))

    def send1(k, i):
        d, m = FOLDS[k][i]
        return rcopy(Sb.at[k, (z + d + m + NZ) % NZ], R1.at[k, i], s1s.at[k, i], s1r.at[k, i], zrow(d), q)

    def row1(k):
        xsend(k).wait_recv()
        s = Rf[k, xl] + Xr[k].astype(F32)
        Sf[k] = s
        Sb[k] = s.astype(BF16)
        for i in range(13):
            go(send1(k, i))

    def folded(k, m):
        u = Sf[k, (z + m + NZ) % NZ]
        mine = [i for i in range(13) if FOLDS[k][i][1] == m]
        for i in mine:
            send1(k, i).wait_recv()
        for i in mine:
            u = u + R1[k, i].astype(F32)
        return u

    def send2(k, i):
        return rcopy(Ub.at[k, i], R2.at[k, i], s2s.at[k, i], s2r.at[k, i], zrow(5 - 10 * i), q)

    def row2(k):
        for i in range(2):
            Ub[k, i] = folded(k, 5 - 10 * i).astype(BF16)
            go(send2(k, i))

    def row3(k, out_ref):
        v = folded(k, 0)
        for i in range(2):
            send2(k, i).wait_recv()
        for i in range(2):
            v = v + R2[k, i].astype(F32)
        out_ref[...] = v.astype(BF16)

    tn = (((0,), (0,)), ((), ()))
    nt = (((1,), (1,)), ((), ()))
    x = gathered(0)
    partial(0, jnp.dot(x, win[...], preferred_element_type=F32))
    g = gathered(1)
    partial(1, lax.dot_general(g, wout[...], nt, preferred_element_type=F32))
    scatter(0)
    scatter(1)
    spread_of(2, (1, 2))
    partial(2, jnp.dot(gathered(2), win[...], preferred_element_type=F32))
    act, slope = gelu_parts(summed(0))
    spread(0, act.astype(BF16))
    spread(1, (summed(1) * slope).astype(BF16))
    scatter(2)
    pass_on(0)
    pass_on(1)
    spread(2, gelu_parts(summed(2))[0].astype(BF16))
    h = whole(1)
    rpartial(0, lax.dot_general(h, win[...], nt, preferred_element_type=F32))
    pass_on(2)
    rpartial(1, jnp.dot(whole(2), wout[...], preferred_element_type=F32))
    gwi[...] = lax.dot_general(
        T[0].astype(F32).reshape(256, 768).astype(BF16), h, tn, preferred_element_type=F32
    ).astype(BF16)
    row1(0)
    gwo[...] = lax.dot_general(
        whole(0), T[1].astype(F32).reshape(256, 768).astype(BF16), tn, preferred_element_type=F32
    ).astype(BF16)
    row1(1)
    row2(0)
    row2(1)
    row3(0, ing_ref)
    row3(1, lay_ref)

    for wait in last:
        wait()


def call(acts, win, wout):
    vm = pl.BlockSpec(memory_space=pltpu.VMEM)
    hbm = pl.BlockSpec(memory_space=pltpu.HBM)
    V = pltpu.VMEM
    D = lambda *s: pltpu.SemaphoreType.DMA(s)
    blk = jax.ShapeDtypeStruct((8, 768), BF16)
    wt = jax.ShapeDtypeStruct((768, 768), BF16)
    return pl.pallas_call(
        kernel,
        out_shape=(blk, blk, wt, wt),
        in_specs=[vm, hbm, hbm],
        out_specs=(vm,) * 4,
        scratch_shapes=[
            V((3, 32, 8, 768), BF16), V((768, 768), BF16), V((768, 768), BF16),
            V((3, 8, 2, 16, 768), F32), V((3, 8, 16, 768), F32),
            V((3, 8, 16, 768), F32), V((3, 8, 16, 768), BF16), V((3, 8, 16, 768), BF16),
            V((3, 8, 2, 16, 768), BF16),
            V((2, 2, 16, 8, 768), F32), V((2, 2, 16, 8, 768), BF16), V((2, 16, 8, 768), BF16),
            V((2, 16, 8, 768), F32), V((2, 16, 8, 768), BF16), V((2, 13, 8, 768), BF16),
            V((2, 2, 8, 768), BF16), V((2, 2, 8, 768), BF16),
            D(2), D(3, 3), D(3, 3), D(3, 13), D(3, 13), D(3, 13), D(3, 16), D(3, 16), D(1),
            D(3), D(3), D(3, 8), D(3, 8), D(3, 8), D(3, 8), D(3, 8), D(3, 8),
            D(2), D(2), D(2, 13), D(2, 13), D(2, 2), D(2, 2),
        ],
        compiler_params=pltpu.CompilerParams(
            collective_id=0, has_side_effects=True, vmem_limit_bytes=51 * 1024 * 1024
        ),
        name="ffn",
    )(acts, win, wout)


def local(tokens, past_tokens, out_grad, w_in, w_out):
    return call(jnp.stack((past_tokens, out_grad, tokens)), w_in, w_out)


def solution(mesh):
    return jax.shard_map(
        local,
        mesh=mesh,
        in_specs=(P("row", "col"), P("row", "col"), P("row", "col"), P("col", "row"), P("row", "col")),
        out_specs=(P("row", "col"), P("row", "col"), P("col", "row"), P("row", "col")),
        check_vma=False,
    )
```

```python
import functools

import jax
import jax.numpy as jnp
from jax import lax
from jax.experimental import pallas as pl
from jax.experimental.pallas import tpu as pltpu
from jax.sharding import PartitionSpec as P

MESH = pl.DeviceIdType.MESH
F32, BF16 = jnp.float32, jnp.bfloat16
NZ = 16


def gelu_parts(pre):
    cdf = 0.5 * (1.0 + lax.erf(pre * 0.7071067811865476))
    slope = cdf + pre * jnp.exp(-0.5 * pre * pre) * 0.3989422804014327
    return (pre * cdf, slope)


SEED = (0, 5, -5)
NEAR = tuple((d, e) for e in range(3) for d in (2, -2, 1, -1))
SPREAD = (NEAR + ((3, 1),), NEAR + ((-3, 2),), NEAR + ((3, 1),))
BOTH = ()
FOLD = tuple((d, m) for m in (5, -5, 0) for d in (2, -2, 1, -1))
FOLDS = (((-3, -5),) + FOLD, ((3, 5),) + FOLD)


def kernel(
    acts_ref, win_hbm, wout_hbm,
    lay_ref, ing_ref, gwi, gwo,
    T, win, wout, Pf, Dr, S8, Cs, Cr, H,
    Rf, Xb, Xr, Sf, Sb, R1, Ub, R2,
    wsem, ass, asr, bss, bsr, bds, axs, axr, lsem,
    dss, drs, css, crs, hss, hrs, hds, hdr,
    xss, xrs, s1s, s1r, s2s, s2r,
):
    r, q = lax.axis_index("row"), lax.axis_index("col")
    xl, z = r // NZ, r % NZ
    ch, c = q // 2, q % 2
    xh, y = ch // 4, ch % 4
    xp = (1 - xl) * NZ + z
    qp = ch * 2 + (1 - c)
    last = []

    def zrow(d, x=xl):
        return x * NZ + (z + d + 2 * NZ) % NZ

    def chip(k, sign=1):
        return ((xh + sign * (k // 4) + 2) % 2) * 4 + (y + sign * (k % 4) + 4) % 4

    def rcopy(src, dst, ss, rs, rr, qq):
        return pltpu.make_async_remote_copy(
            src_ref=src, dst_ref=dst, send_sem=ss, recv_sem=rs, device_id=(rr, qq), device_id_type=MESH
        )

    def go(cp):
        cp.start()
        last.append(cp.wait_send)

    loc = pltpu.make_async_copy(acts_ref, T.at[:, r], lsem.at[0])
    loc.start()
    cw1 = pltpu.make_async_copy(win_hbm, win, wsem.at[0])
    cw2 = pltpu.make_async_copy(wout_hbm, wout, wsem.at[1])
    cw1.start()
    cw2.start()

    barrier = pltpu.get_barrier_semaphore()
    rows = [zrow(d) for d in (1, -1, 2, -2, 3, -3, 5, -5)] + [zrow(d, 1 - xl) for d in (0, 2, -2, 3, -3)]
    for rr in rows:
        pl.semaphore_signal(barrier, inc=1, device_id=(rr, q), device_id_type=MESH)
    for qq in [chip(k) * 2 + c for k in range(1, 8)] + [qp]:
        pl.semaphore_signal(barrier, inc=1, device_id=(r, qq), device_id_type=MESH)
    pl.semaphore_wait(barrier, 21)

    def xcopy(src, a, d):
        zz = (z + d + 2 * NZ) % NZ
        slot = xl * NZ + zz
        return rcopy(src, T.at[a, slot], axs.at[a, zz], axr.at[a, zz], xp, q)

    def acopy(src, a, e, e2, d):
        slot = zrow(SEED[e])
        return rcopy(src, T.at[a, slot], ass.at[a, e2], asr.at[a, e2], zrow(d), q)

    def arecv(a, e2):
        slot = zrow(SEED[e2])
        acopy(T.at[a, slot], a, e2, e2, 5).wait_recv()

    def bcopy(src, a, i):
        d, e = SPREAD[a][i]
        slot = zrow(SEED[e])
        return rcopy(src, T.at[a, slot], bss.at[a, i], bsr.at[a, i], zrow(-d), q)

    def bcross(src, a, i):
        d, e = SPREAD[a][i]
        zz = (z + SEED[e] + 2 * NZ) % NZ
        slot = zrow(SEED[e])
        return rcopy(src, T.at[a, slot], bds.at[a, i], axr.at[a, zz], zrow(-d, 1 - xl), q)

    def brecv(a, i):
        d, e = SPREAD[a][i]
        slot = zrow(d + SEED[e])
        rcopy(T.at[a, slot], T.at[a, slot], bss.at[a, i], bsr.at[a, i], zrow(-d), q).wait_recv()
        if i not in BOTH:
            go(xcopy(T.at[a, slot], a, d + SEED[e]))

    def seeded(a, e):
        src = acts_ref.at[a] if e == 0 else T.at[a, zrow(SEED[e])]
        if e == 0:
            go(acopy(src, a, 0, 1, -5))
            go(acopy(src, a, 0, 2, 5))
        for i in sorted(range(13), key=lambda i: -abs(SPREAD[a][i][0])):
            if SPREAD[a][i][1] == e:
                go(bcopy(src, a, i))
                if i in BOTH:
                    go(bcross(src, a, i))
        go(xcopy(src, a, SEED[e]))

    def spread_of(a, es):
        for i, (d, e) in enumerate(SPREAD[a]):
            if e in es:
                brecv(a, i)

    for a in range(2):
        seeded(a, 0)
    for a in range(2):
        spread_of(a, (0,))
    for a in range(2):
        for e in (1, 2):
            arecv(a, e)
            seeded(a, e)
    seeded(2, 0)
    for a in range(2):
        spread_of(a, (1, 2))
    spread_of(2, (0,))
    for e in (1, 2):
        arecv(2, e)
        seeded(2, e)

    cw1.wait()
    cw2.wait()
    loc.wait()

    def gathered(a):
        @pl.loop(0, NZ)
        def _(zz):
            slot = (1 - xl) * NZ + zz
            rcopy(T.at[a, slot], T.at[a, slot], axs.at[a, zz], axr.at[a, zz], xp, q).wait_recv()

        return T[a].astype(F32).reshape(256, 768).astype(BF16)

    def d2d(k):
        return rcopy(Pf.at[k, :, 1 - c], Dr.at[k], dss.at[k], drs.at[k], r, qp)

    def partial(k, part):
        Pf[k] = part.reshape(8, 2, 16, 768)
        go(d2d(k))

    def csend(k, j):
        return rcopy(Cs.at[k, chip(j)], Cr.at[k, j], css.at[k, j], crs.at[k, j], r, chip(j) * 2 + c)

    def scatter(k):
        d2d(k).wait_recv()
        sums = Pf[k, :, c] + Dr[k]
        S8[k] = sums
        Cs[k] = sums.astype(BF16)
        for j in (6, 2, 4, 5, 7, 1, 3):
            go(csend(k, j))

    def summed(k):
        total = S8[k, ch]
        for j in range(1, 8):
            csend(k, j).wait_recv()
        for j in range(1, 8):
            total = total + Cr[k, j].astype(F32)
        return total

    def hcopy(k, owner, j, ss, rs, core, qq):
        ref = H.at[k, owner, core]
        return rcopy(ref, ref, ss.at[k, j], rs.at[k, j], r, qq)

    def spread(k, value):
        H[k, ch, c] = value
        for j in (6, 2, 4, 5, 7, 1, 3):
            go(hcopy(k, ch, j, hss, hrs, c, chip(j) * 2 + c))
        go(hcopy(k, ch, 0, hds, hdr, c, qp))

    def pass_on(k):
        for j in (1, 3, 4, 2, 5, 7, 6):
            hcopy(k, chip(j, -1), j, hss, hrs, c, qp).wait_recv()
            go(hcopy(k, chip(j, -1), j, hds, hdr, c, qp))

    def whole(k):
        for j in range(8):
            hcopy(k, chip(j, -1), j, hds, hdr, 1 - c, qp).wait_recv()
        return H[k].reshape(256, 768)

    def xsend(k):
        return rcopy(Xb.at[k, 1 - xl], Xr.at[k], xss.at[k], xrs.at[k], xp, q)

    def rpartial(k, part):
        for f in range(2):
            half = part[:, 384 * f : 384 * f + 384].reshape(2, NZ, 8, 384)
            Rf[2 * k + f] = half
            Xb[2 * k + f] = half.astype(BF16)
            go(xsend(2 * k + f))

    def send1(k, i):
        d, m = FOLDS[k % 2][i]
        return rcopy(Sb.at[k, (z + d + m + NZ) % NZ], R1.at[k, i], s1s.at[k, i], s1r.at[k, i], zrow(d), q)

    def row1(k):
        xsend(k).wait_recv()
        s = Rf[k, xl] + Xr[k].astype(F32)
        Sf[k] = s
        Sb[k] = s.astype(BF16)
        for i in range(13):
            go(send1(k, i))

    def folded(k, m):
        u = Sf[k, (z + m + NZ) % NZ]
        mine = [i for i in range(13) if FOLDS[k % 2][i][1] == m]
        for i in mine:
            send1(k, i).wait_recv()
        for i in mine:
            u = u + R1[k, i].astype(F32)
        return u

    def send2(k, i):
        return rcopy(Ub.at[k, i], R2.at[k, i], s2s.at[k, i], s2r.at[k, i], zrow(5 - 10 * i), q)

    def row2(k):
        for i in range(2):
            Ub[k, i] = folded(k, 5 - 10 * i).astype(BF16)
            go(send2(k, i))

    def row3(k, out_ref):
        v = folded(k, 0)
        for i in range(2):
            send2(k, i).wait_recv()
        for i in range(2):
            v = v + R2[k, i].astype(F32)
        out_ref[:, 384 * (k % 2) : 384 * (k % 2) + 384] = v.astype(BF16)

    tn = (((0,), (0,)), ((), ()))
    nt = (((1,), (1,)), ((), ()))
    x = gathered(0)
    partial(0, jnp.dot(x, win[...], preferred_element_type=F32))
    g = gathered(1)
    partial(1, lax.dot_general(g, wout[...], nt, preferred_element_type=F32))
    scatter(0)
    scatter(1)
    spread_of(2, (1, 2))
    partial(2, jnp.dot(gathered(2), win[...], preferred_element_type=F32))
    act, slope = gelu_parts(summed(0))
    spread(1, (summed(1) * slope).astype(BF16))
    scatter(2)
    pass_on(1)
    spread(2, gelu_parts(summed(2))[0].astype(BF16))
    spread(0, act.astype(BF16))
    h = whole(1)
    rpartial(0, lax.dot_general(h, win[...], nt, preferred_element_type=F32))
    pass_on(2)
    rpartial(1, jnp.dot(whole(2), wout[...], preferred_element_type=F32))
    pass_on(0)
    row1(0)
    row1(1)
    gwi[...] = lax.dot_general(
        T[0].astype(F32).reshape(256, 768).astype(BF16), h, tn, preferred_element_type=F32
    ).astype(BF16)
    row1(2)
    row1(3)
    row2(0)
    row2(1)
    gwo[...] = lax.dot_general(
        whole(0), T[1].astype(F32).reshape(256, 768).astype(BF16), tn, preferred_element_type=F32
    ).astype(BF16)
    row2(2)
    row2(3)
    row3(0, ing_ref)
    row3(1, ing_ref)
    row3(2, lay_ref)
    row3(3, lay_ref)

    for wait in last:
        wait()


def call(acts, win, wout):
    vm = pl.BlockSpec(memory_space=pltpu.VMEM)
    hbm = pl.BlockSpec(memory_space=pltpu.HBM)
    V = pltpu.VMEM
    D = lambda *s: pltpu.SemaphoreType.DMA(s)
    blk = jax.ShapeDtypeStruct((8, 768), BF16)
    wt = jax.ShapeDtypeStruct((768, 768), BF16)
    return pl.pallas_call(
        kernel,
        out_shape=(blk, blk, wt, wt),
        in_specs=[vm, hbm, hbm],
        out_specs=(vm,) * 4,
        scratch_shapes=[
            V((3, 32, 8, 768), BF16), V((768, 768), BF16), V((768, 768), BF16),
            V((3, 8, 2, 16, 768), F32), V((3, 8, 16, 768), F32),
            V((3, 8, 16, 768), F32), V((3, 8, 16, 768), BF16), V((3, 8, 16, 768), BF16),
            V((3, 8, 2, 16, 768), BF16),
            V((4, 2, 16, 8, 384), F32), V((4, 2, 16, 8, 384), BF16), V((4, 16, 8, 384), BF16),
            V((4, 16, 8, 384), F32), V((4, 16, 8, 384), BF16), V((4, 13, 8, 384), BF16),
            V((4, 2, 8, 384), BF16), V((4, 2, 8, 384), BF16),
            D(2), D(3, 3), D(3, 3), D(3, 13), D(3, 13), D(3, 13), D(3, 16), D(3, 16), D(1),
            D(3), D(3), D(3, 8), D(3, 8), D(3, 8), D(3, 8), D(3, 8), D(3, 8),
            D(4), D(4), D(4, 13), D(4, 13), D(4, 2), D(4, 2),
        ],
        compiler_params=pltpu.CompilerParams(
            collective_id=0, has_side_effects=True, vmem_limit_bytes=51 * 1024 * 1024
        ),
        name="ffn",
    )(acts, win, wout)


def local(tokens, past_tokens, out_grad, w_in, w_out):
    return call(jnp.stack((past_tokens, out_grad, tokens)), w_in, w_out)


def solution(mesh):
    return jax.shard_map(
        local,
        mesh=mesh,
        in_specs=(P("row", "col"), P("row", "col"), P("row", "col"), P("col", "row"), P("row", "col")),
        out_specs=(P("row", "col"), P("row", "col"), P("col", "row"), P("row", "col")),
        check_vma=False,
    )
```
